256 devices in a mesh: bank: 64 (over z, y, core), zero: 4 (over x).
Axes of the slice: x: 4, y: 4, z: 8, core: 2. Of those that a mesh axis runs over, the one named last changes fastest.
Arguments:
- train_down: float32 [128, 768, 2048], P('bank', None, 'zero'), may hold values from -0.3125 to 0.3125
- other_down: float32 [128, 768, 2048], P('bank', None, 'zero'), may hold values from -0.21875 to 0.21875
- router_weight: float32 [2048, 128], P('zero', 'bank'), may hold values from -0.125 to 0.125
- router_gain: float32 [2048], P('zero'), may hold values from 0.25 to 1.75
Outputs:
- ready_down: bfloat16 [128, 768, 2048], P('bank')
- scale_down: float32 [128, 768], P('bank')
- serve_router: bfloat16 [2048, 128], replicated
- latest_down: float32 [128, 768, 2048], P('bank', None, 'zero')
The draws below stay inside these ranges and needn't reach their ends.
All inputs are finite; a program needn't handle non-finite values. Where the reference program divides by a largest or mean magnitude, that divisor is 1e-20 or more.
Results may differ from the reference program's by a relative error of at most 0.001.
Values may be sent and summed in bfloat16 or wider, within the bound.
No kernel may reach another device: no remote copies, remote signals or barrier semaphores. Data moves between devices by JAX's collectives and lax.ppermute only.
A program may use at most 128 MiB of HBM per device.

```python
import jax
import jax.numpy as jnp

EXPERTS = 128
D_MODEL = 2048
D_EXPERT = 768


def spiked(drawn, rng, source, target, shards_of, factor):
    def block_of(dim):
        return (jnp.arange(drawn.shape[dim]) // (drawn.shape[dim] // shards_of)).reshape((-1,) + (1,) * (drawn.ndim - 1 - dim))

    first = jax.random.permutation(rng, shards_of)[block_of(target)]
    second = (block_of(target) + shards_of // 2) % shards_of
    return jnp.where((block_of(source) == first) | (block_of(source) == second), factor * drawn, drawn)


def shard_levels(stream_key, extent, pieces, smallest, high):
    gain, own = 1.0, jax.random.fold_in(stream_key, 6)
    for axis_at, blocks in pieces:
        draws = jnp.exp(jax.random.uniform(jax.random.fold_in(own, axis_at), (blocks,), jnp.float32, smallest / len(pieces), high / len(pieces)))
        gain = gain * jnp.repeat(draws, extent[axis_at] // blocks).reshape([-1 if axis == axis_at else 1 for axis in range(len(extent))])
    return gain


def gaussian(key, extent, width, most, pieces=(), kind=jnp.bfloat16):
    entries = width * jax.random.normal(key, extent, jnp.float32)
    if pieces:
        entries = entries * shard_levels(key, extent, pieces, -0.22, 0.18)
    return jnp.clip(entries, -most, most).astype(kind)


def noise_with(own_key, extent, spread, bound, shards, heavy, held_as=jnp.bfloat16):
    entries = spread * jax.random.normal(own_key, extent, jnp.float32)
    if shards:
        entries = entries * shard_levels(own_key, extent, shards, -0.22, 0.18)
    return jnp.clip(spiked(entries, jax.random.fold_in(own_key, 3), *heavy), -bound, bound).astype(held_as)


def setup_inputs(seed: int = 0) -> dict:
    arg_keys = jax.random.split(jax.random.key(seed), 5)
    train_down = noise_with(arg_keys[0], (EXPERTS, D_EXPERT, D_MODEL), D_EXPERT ** -0.5, 0.3125, ((0, 64), (2, 4)), (2, 1, 4, 2.0), jnp.float32)
    other_down = gaussian(arg_keys[1], (EXPERTS, D_EXPERT, D_MODEL), D_EXPERT ** -0.5, 0.21875, ((0, 64), (2, 4)), jnp.float32)
    router_weight = gaussian(arg_keys[2], (D_MODEL, EXPERTS), D_MODEL ** -0.5, 0.125, ((0, 4), (1, 64)), jnp.float32)
    router_gain = jnp.clip(1.0 + 0.15 * jax.random.normal(arg_keys[3], (D_MODEL,), jnp.float32), 0.25, 1.75)
    return {"train_down": train_down, "other_down": other_down, "router_weight": router_weight, "router_gain": router_gain}


def reference(train_down, other_down, router_weight, router_gain):
    latest_down = 0.5 * other_down + 0.5 * train_down
    scale_down = jnp.sum(jnp.abs(latest_down), axis=2) / D_MODEL
    ready_down = (latest_down / jnp.expand_dims(scale_down, 2)).astype(jnp.bfloat16)
    serve_router = (router_weight * router_gain[:, None]).astype(jnp.bfloat16)
    return ready_down, scale_down, serve_router, latest_down
```

```python
import functools

import jax
import jax.numpy as jnp
from jax import lax
from jax.experimental import pallas as pl
from jax.experimental.pallas import tpu as pltpu
from jax.sharding import Mesh
from jax.sharding import PartitionSpec as P

D_MODEL = 2048
SIDES = 4
BANK = ("bank_0", "bank_1", "bank_2")


def shifted(x, by):
    return lax.ppermute(x, "zero", [(k, (k + by) % SIDES) for k in range(SIDES)])


def placed_into(shape, pieces, where, into=None):
    count = len(pieces)

    def kernel(*refs):
        src, out, sem = refs[:count], refs[-2], refs[-1]
        me = lax.axis_index("zero")
        copies = []
        for at, (expert, behind) in enumerate(where):
            width = src[at].shape[-1]
            col = pl.multiple_of(lax.rem(me - behind + SIDES, SIDES) * width, 512)
            copies.append(
                pltpu.make_async_copy(src[at], out.at[expert, :, pl.ds(col, width)], sem.at[at])
            )
        for copy in copies:
            copy.start()
        for copy in copies:
            copy.wait()

    args = list(pieces) + ([] if into is None else [into])
    specs = [pl.BlockSpec(memory_space=pl.ANY)] * count
    if into is not None:
        specs.append(pl.BlockSpec(memory_space=pltpu.HBM))
    size = sum(p.size * 2 for p in pieces)
    return pl.pallas_call(
        kernel,
        out_shape=jax.ShapeDtypeStruct(shape, jnp.bfloat16),
        in_specs=specs,
        out_specs=pl.BlockSpec(memory_space=pltpu.HBM),
        scratch_shapes=[pltpu.SemaphoreType.DMA((count,))],
        input_output_aliases={} if into is None else {count: 0},
        compiler_params=pltpu.CompilerParams(vmem_limit_bytes=1 << 20),
        cost_estimate=pl.CostEstimate(flops=size, bytes_accessed=2 * size, transcendentals=0),
        name="place",
    )(*args)


def shards(train_down, other_down, router_weight, router_gain):
    latest_down = 0.5 * other_down + 0.5 * train_down
    part = jnp.sum(jnp.abs(latest_down), axis=2)
    total = part + shifted(part, 1) + shifted(part, 2) + shifted(part, 3)
    scale_down = total / D_MODEL
    narrow = [
        (latest_down[e] / scale_down[e][:, None]).astype(jnp.bfloat16) for e in range(2)
    ]
    from_left = {0: shifted(narrow[0], 1)}
    from_right = {1: shifted(narrow[1], -1)}
    from_left[1] = shifted(narrow[1], 1)
    from_right[0] = shifted(narrow[0], -1)
    far0 = shifted(from_left[0], 1)
    far1 = shifted(from_right[1], -1)
    shape = (2, narrow[0].shape[0], D_MODEL)
    ready = placed_into(
        shape,
        [narrow[0], narrow[1], from_left[0], from_right[1], from_left[1], from_right[0]],
        [(0, 0), (1, 0), (0, 1), (1, -1), (1, 1), (0, -1)],
    )
    ready = placed_into(shape, [far0, far1], [(0, 2), (1, 2)], ready)

    part_router = (router_weight * router_gain[:, None]).astype(jnp.bfloat16)
    row_router = lax.all_gather(part_router.T, "zero", axis=1, tiled=True)
    every = lax.all_gather(row_router, ("bank_0", "bank_1", "bank_2"), axis=0, tiled=True)
    serve_router = every.T
    return (ready, scale_down, serve_router, latest_down)


def solution(mesh):
    split = Mesh(
        mesh.devices.reshape(8, 4, 2, mesh.shape["zero"]), ("bank_0", "bank_1", "bank_2", "zero")
    )
    placed = (P(BANK, None, "zero"), P(BANK, None, "zero"), P("zero", BANK), P("zero"))
    return jax.shard_map(
        shards,
        mesh=split,
        in_specs=placed,
        out_specs=(P(BANK, None, None), P(BANK, None), P(), P(BANK, None, "zero")),
        check_vma=False,
    )
```

```python
import jax
import jax.numpy as jnp
from jax import lax
from jax.experimental import pallas as pl
from jax.experimental.pallas import tpu as pltpu
from jax.sharding import Mesh
from jax.sharding import PartitionSpec as P

D_MODEL = 2048
BANK = ("bank_0", "bank_1", "bank_2")


def shifted(x, axis, by):
    n = lax.axis_size(axis)
    return lax.ppermute(x, axis, [(k, (k + by) % n) for k in range(n)])


def in_turn(x, axis):
    n = lax.axis_size(axis)
    return [x] + [shifted(x, axis, -by) for by in range(1, n)]


def ordered(blocks, axis):
    n = lax.axis_size(axis)
    at = lax.axis_index(axis)
    full = jnp.zeros((n, *blocks[0].shape), blocks[0].dtype)
    for by, block in enumerate(blocks):
        full = lax.dynamic_update_index_in_dim(full, block, lax.rem(at + by, n), 0)
    return full


def placed_into(shape, pieces, where, into=None):
    count = len(pieces)

    def kernel(*refs):
        src, out = refs[:count], refs[-2 - count - 1]
        held, came, went = refs[-2 - count : -2], refs[-2], refs[-1]
        me, sides = lax.axis_index("zero"), lax.axis_size("zero")
        copies = []
        for at, (expert, behind) in enumerate(where):
            width = src[at].shape[-1]
            col = pl.multiple_of(lax.rem(me - behind + sides, sides) * width, width)
            copies.append(
                (
                    pltpu.make_async_copy(src[at], held[at], came.at[at]),
                    pltpu.make_async_copy(
                        held[at], out.at[expert, :, pl.ds(col, width)], went.at[at]
                    ),
                )
            )
        for come, _ in copies:
            come.start()
        for come, go in copies:
            come.wait()
            go.start()
        for _, go in copies:
            go.wait()

    args = list(pieces) + ([] if into is None else [into])
    specs = [pl.BlockSpec(memory_space=pl.ANY)] * count
    if into is not None:
        specs.append(pl.BlockSpec(memory_space=pltpu.HBM))
    size = sum(p.size * 2 for p in pieces)
    return pl.pallas_call(
        kernel,
        out_shape=jax.ShapeDtypeStruct(shape, jnp.bfloat16),
        in_specs=specs,
        out_specs=pl.BlockSpec(memory_space=pltpu.HBM),
        scratch_shapes=[pltpu.VMEM(p.shape, p.dtype) for p in pieces]
        + [pltpu.SemaphoreType.DMA((count,)), pltpu.SemaphoreType.DMA((count,))],
        input_output_aliases={} if into is None else {count: 0},
        compiler_params=pltpu.CompilerParams(vmem_limit_bytes=size + (1 << 20)),
        cost_estimate=pl.CostEstimate(flops=size, bytes_accessed=2 * size, transcendentals=0),
        name="place",
    )(*args)


def work(train_down, other_down, router_weight, router_gain):
    part_router = (router_weight * router_gain[:, None]).astype(jnp.bfloat16).T
    latest_down = 0.5 * other_down + 0.5 * train_down
    part = jnp.sum(jnp.abs(latest_down), axis=2)
    rows = part.shape[1]
    message = jnp.concatenate([part, part_router.astype(jnp.float32)], axis=1)
    messages = in_turn(message, "zero")
    total = sum(m[:, :rows] for m in messages)
    scale_down = total / D_MODEL
    narrow = [
        (latest_down[e] / scale_down[e][:, None]).astype(jnp.bfloat16) for e in range(2)
    ]
    left0 = shifted(narrow[0], "zero", 1)
    right1 = shifted(narrow[1], "zero", -1)
    left1 = shifted(narrow[1], "zero", 1)
    right0 = shifted(narrow[0], "zero", -1)
    far0 = shifted(left0, "zero", 1)
    far1 = shifted(right1, "zero", -1)
    shape = (2, rows, D_MODEL)
    ready = placed_into(
        shape,
        [narrow[0], narrow[1], left0, right1, left1, right0],
        [(0, 0), (1, 0), (0, 1), (1, -1), (1, 1), (0, -1)],
    )
    ready = placed_into(shape, [far0, far1], [(0, 2), (1, 2)], ready)

    row_router = ordered([m[:, rows:].astype(jnp.bfloat16) for m in messages], "zero")
    line = ordered(in_turn(row_router, "bank_0"), "bank_0")
    plane = ordered(in_turn(line, "bank_1"), "bank_1")
    every = ordered(in_turn(plane, "bank_2"), "bank_2")
    serve_router = every.transpose(3, 5, 2, 1, 0, 4).reshape(D_MODEL, -1)
    return (ready, scale_down, serve_router, latest_down)


def solution(mesh):
    split = Mesh(
        mesh.devices.reshape(8, 4, 2, mesh.shape["zero"]), ("bank_0", "bank_1", "bank_2", "zero")
    )
    placed = (P(BANK, None, "zero"), P(BANK, None, "zero"), P("zero", BANK), P("zero"))
    return jax.shard_map(
        work,
        mesh=split,
        in_specs=placed,
        out_specs=(P(BANK, None, None), P(BANK, None), P(), P(BANK, None, "zero")),
        check_vma=False,
    )
```
